32 devices in a mesh: gx: 8 (over z, y), gy: 4 (over x, core).
Axes of the slice: x: 2, y: 2, z: 4, core: 2. Of those that a mesh axis runs over, the one named last changes fastest.
Arguments:
- anomalies: float32 [80, 16, 32, 128], P(None, 'gx', 'gy'), may hold values from -6 to 6
- state_mean: float32 [16, 32, 128], P('gx', 'gy'), may hold values from -6 to 6
- obs_value: float32 [16, 256], P(None, 'gy'), may hold values from -8 to 8
- obs_cell: int32 [16, 256], replicated, may hold values from 0 to 2047
- owner: int32 [16], replicated, may hold values from 0 to 7, as said below
- order: int32 [16], replicated, may hold values from 0 to 15, each once
- root_inv: float32 [16, 256, 256], P(None, 'gy'), as said below
- gain_inv: float32 [16, 256, 256], P(None, 'gy'), as said below
Outputs:
- post_anomalies: float32 [80, 16, 32, 128], P(None, 'gx', 'gy')
- post_mean: float32 [16, 32, 128], P('gx', 'gy')
The draws below stay inside these ranges and needn't reach their ends.
Inputs may be any that keep to these rules, and one draw needn't show every extreme that they name: `owner`: some batch lies at slab 8 - 2, some at slab 1 and some at slab 8 // 2; the others favour low slabs. `order`: each batch number once. `root_inv`: symmetric. `gain_inv`: symmetric.
All inputs are finite; a program needn't handle non-finite values.
Results may differ from the reference program's by a relative error of at most 0.0001.
Values sent between devices are 32-bit elements; how exact they have to be, the bound alone decides.
A program may use at most 64 MiB of HBM per device.

```python
import math
import jax
import jax.numpy as jnp
from jax import lax

MEMBERS = 80
OBS = 256
BATCHES = 16
LON_DEV = 2
LAT_DEV = 8
LEVELS = 128
REACH = 3
NLON = 16
NLAT = 32
CELLS = 2048
N_GX = 8
N_GY = 4


def inverse_table(key, floor_value, top_value):
    key_diag, key_off = jax.random.split(key, 2)
    diagonal = jnp.exp(jax.random.uniform(key_diag, (BATCHES, OBS), jnp.float32, math.log(floor_value), math.log(top_value)))
    spread = 0.6 * math.sqrt(floor_value * top_value) / math.sqrt(OBS)
    offdiag_noise = jax.random.normal(key_off, (BATCHES, OBS, OBS), jnp.float32) * spread
    inverse = 0.5 * (offdiag_noise + jnp.swapaxes(offdiag_noise, 1, 2)) + diagonal[:, :, None] * jnp.eye(OBS, dtype=jnp.float32)
    return inverse


def draw_root_inv(key, part):
    return inverse_table(jax.random.fold_in(key, 11), 0.15, 0.5)


def draw_gain_inv(key, part):
    return inverse_table(jax.random.fold_in(key, 23), 0.3, 0.9)


def draw_owner(key, part):
    key_first, key_second, key_perm = jax.random.split(jax.random.fold_in(key, 37), 3)
    first_draw = jax.random.randint(key_first, (BATCHES,), 0, N_GX, dtype=jnp.int32)
    second_draw = jax.random.randint(key_second, (BATCHES,), 0, N_GX, dtype=jnp.int32)
    slabs = jnp.minimum(first_draw, second_draw)
    anchors = jnp.array([N_GX - 2, 1, N_GX // 2], dtype=jnp.int32)
    slabs = slabs.at[:3].set(anchors)
    shuffle = jax.random.permutation(key_perm, BATCHES)
    return slabs[shuffle].astype(jnp.int32)


def place_ends(drawn, own_key, least, high):
    index_at = [jax.random.randint(jax.random.fold_in(own_key, axis), (), 0, length) for axis, length in enumerate(drawn.shape)]
    longest = drawn.shape.index(max(drawn.shape))
    neighbour = index_at[:longest] + [(index_at[longest] + 1) % drawn.shape[longest]] + index_at[longest + 1:]
    return drawn.at[tuple(index_at)].set(least).at[tuple(neighbour)].set(high)


def block_levels(own_key, shape, cuts, low, largest):
    loudness = 1.0
    for dim, parts in cuts:
        draws = jax.random.uniform(jax.random.fold_in(jax.random.fold_in(own_key, 6), dim), (parts,), jnp.float32, low / len(cuts), largest / len(cuts))
        loudness = loudness * jnp.repeat(jnp.exp(draws), shape[dim] // parts).reshape((-1,) + (1,) * (len(shape) - 1 - dim))
    return loudness


def noise(key, dims, deviation, most, shards=(), kind=jnp.bfloat16):
    level = block_levels(key, dims, shards, -0.22, 0.18) if shards else 1.0
    drawn = jax.random.normal(key, dims, jnp.float32) * deviation * level
    return jnp.minimum(jnp.maximum(drawn, -most), most).astype(kind)


def setup_inputs(seed: int = 0) -> dict:
    arg_keys = jax.random.split(jax.random.key(seed), 9)
    anomalies = noise(arg_keys[0], (MEMBERS, NLON, NLAT, LEVELS), 1.0, 6.0, ((1, 8), (2, 4)), jnp.float32)
    state_mean = noise(arg_keys[1], (NLON, NLAT, LEVELS), 1.0, 6.0, ((0, 8), (1, 4)), jnp.float32)
    obs_value = noise(arg_keys[2], (BATCHES, OBS), 1.5, 8.0, ((1, 4),), jnp.float32)
    obs_cell = place_ends(jax.random.randint(arg_keys[3], (BATCHES, OBS), 0, CELLS), jax.random.fold_in(arg_keys[3], 1), 0, CELLS - 1).astype(jnp.int32)
    owner = draw_owner(jax.random.fold_in(arg_keys[8], 71), 0)
    order = jax.random.permutation(arg_keys[5], BATCHES).astype(jnp.int32)
    root_inv = draw_root_inv(jax.random.fold_in(arg_keys[8], 71), 0)
    gain_inv = draw_gain_inv(jax.random.fold_in(arg_keys[8], 71), 0)
    return {"anomalies": anomalies, "state_mean": state_mean, "obs_value": obs_value, "obs_cell": obs_cell, "owner": owner, "order": order, "root_inv": root_inv, "gain_inv": gain_inv}


def product(left_side, right_side):
    return jnp.dot(left_side, right_side, precision=lax.Precision.HIGHEST, preferred_element_type=jnp.float32)


def reference(anomalies, state_mean, obs_value, obs_cell, owner, order, root_inv, gain_inv):
    lon_total = LON_DEV * N_GX
    lat_total = LAT_DEV * N_GY
    quarter = OBS // N_GY
    window_width = (2 * REACH + 1) * LON_DEV
    reach_cells = REACH * LON_DEV
    taper_span = REACH * LON_DEV + 1.0
    obs_band = jnp.arange(OBS, dtype=jnp.int32) // quarter
    lat_index = jnp.arange(lat_total, dtype=jnp.int32)
    offsets = jnp.arange(window_width, dtype=jnp.int32)

    def assimilate(batch_turn, carried):
        state_field, mean_field = carried
        batch_id = order[batch_turn]
        root_slab = owner[batch_id]
        cells_of = obs_cell[batch_id]
        obs_lon = root_slab * LON_DEV + cells_of // (LAT_DEV * LEVELS)
        obs_lat = obs_band * LAT_DEV + (cells_of // LEVELS) % LAT_DEV
        obs_lev = cells_of % LEVELS
        prior_all = state_field[:, obs_lon, obs_lat, obs_lev]
        innovation = obs_value[batch_id] - mean_field[obs_lon, obs_lat, obs_lev]
        weighted = product(prior_all, root_inv[batch_id].T)
        gain_vec = product(gain_inv[batch_id], innovation)
        window_lon = (root_slab * LON_DEV - reach_cells + offsets) % lon_total
        window = state_field[:, window_lon].reshape(MEMBERS, -1)
        mean_window = mean_field[window_lon].reshape(-1)
        cell_lon = jnp.broadcast_to(window_lon[:, None, None], (window_width, lat_total, LEVELS)).reshape(-1)
        cell_lat = jnp.broadcast_to(lat_index[None, :, None], (window_width, lat_total, LEVELS)).reshape(-1)
        lon_gap = jnp.abs(obs_lon[:, None] - cell_lon[None, :])
        cycle_gap = jnp.minimum(lon_gap, lon_total - lon_gap)
        lat_gap = jnp.abs(obs_lat[:, None] - cell_lat[None, :])
        taper_rows = jnp.maximum(0.0, 1.0 - cycle_gap.astype(jnp.float32) / taper_span) * (1.0 - lat_gap.astype(jnp.float32) / lat_total)
        covariance = product(prior_all.T, window) / (MEMBERS - 1.0)
        gained = taper_rows * covariance
        stacked = jnp.concatenate([weighted, gain_vec[None, :]], axis=0)
        increment = product(stacked, gained)
        new_window = (window - increment[:MEMBERS]).reshape(MEMBERS, window_width, lat_total, LEVELS)
        new_mean = (mean_window + increment[MEMBERS]).reshape(window_width, lat_total, LEVELS)
        state_field = state_field.at[:, window_lon].set(new_window)
        mean_field = mean_field.at[window_lon].set(new_mean)
        return state_field, mean_field

    post_anomalies, post_mean = lax.fori_loop(0, BATCHES, assimilate, (anomalies, state_mean))
    return post_anomalies, post_mean
```

```python
import functools

import jax
import jax.numpy as jnp
from jax import lax
from jax.experimental import pallas as pl
from jax.experimental.pallas import tpu as pltpu
from jax.sharding import PartitionSpec as P

REACH = 3
LANES = 128
MESH = pl.DeviceIdType.MESH
VMEM = pl.BlockSpec(memory_space=pltpu.VMEM)
SMEM = pl.BlockSpec(memory_space=pltpu.SMEM)
F32 = jnp.float32
BF16 = jnp.bfloat16


def split(value):
    high = value.astype(BF16)
    return high, (value - high.astype(F32)).astype(BF16)


def nn(left, right):
    return lax.dot_general(left, right, (((1,), (0,)), ((), ())), preferred_element_type=F32)


def nt(left, right):
    return lax.dot_general(left, right, (((1,), (1,)), ((), ())), preferred_element_type=F32)


def lane_ids(shape):
    return lax.broadcasted_iota(jnp.int32, shape, len(shape) - 1)


def pick_kernel(lon_dev, lat_dev, cells_ref, value_ref, owned_ref, anom_ref, mean_ref, state_ref, rows_ref):
    column, band = lax.axis_index("gx"), lax.axis_index("gy")
    members, classes, levels = anom_ref.shape
    batches, quarter = value_ref.shape

    for c in range(classes):
        lat = (band * lat_dev + c % lat_dev).astype(F32)
        lon = (column * lon_dev + c // lat_dev).astype(F32)
        tall = jnp.concatenate(
            [
                anom_ref[:, c, :],
                mean_ref[pl.ds(c, 1), :],
                jnp.full((1, levels), lat, F32),
                jnp.full((1, levels), lon, F32),
                jnp.zeros((LANES - members - 3, levels), F32),
            ],
            axis=0,
        )
        state_ref[pl.ds(c * levels, levels), :] = tall.T

    lane = lane_ids((1, LANES))

    def batch(t, _):
        mine = owned_ref[t] == column

        @pl.when(mine)
        def _():
            def group(i, _):
                for k in range(8):
                    j = i * 8 + k
                    row = state_ref[pl.ds(cells_ref[t, j], 1), :]
                    rows_ref[pl.ds(t * quarter + j, 1), :] = jnp.where(lane == members + 3, value_ref[t, j], row)
                return 0

            lax.fori_loop(0, quarter // 8, group, 0)

        @pl.when(jnp.logical_not(mine))
        def _():
            rows_ref[pl.ds(pl.multiple_of(t * quarter, quarter), quarter), :] = jnp.zeros((quarter, LANES), F32)

        return 0

    lax.fori_loop(0, batches, batch, 0)


def main_kernel(
    sizes, order_ref, state_ref, obs_ref, lat_ref, lon_ref, root_ref, gain_ref,
    anom_out, mean_out,
    cells_s, obs_s, v_s, vw_s, z3_s, gh_s, gl_s, send_sem, recv_sem,
):
    members, lon_dev, lat_dev, levels, lon_total, lat_total, span, bands = sizes
    batches, _, obs = lat_ref.shape
    quarter = obs // bands
    column, band = lax.axis_index("gx"), lax.axis_index("gy")
    classes = lon_dev * lat_dev
    chunk = 4

    barrier = pltpu.get_barrier_semaphore()
    for k in range(1, bands):
        pl.semaphore_signal(barrier, inc=1, device_id={"gy": lax.rem(band + k, bands)}, device_id_type=MESH)
    pl.semaphore_wait(barrier, bands - 1)

    def widen(value, with_low_in_middle):
        high, low = split(value)
        high, low = high.astype(F32), low.astype(F32)
        second, third = (low, high) if with_low_in_middle else (high, low)
        lane = lane_ids(value.shape)
        room = LANES - members
        moved = pltpu.roll(second, members, 1)
        first = jnp.where(lane < members, high, moved)
        last = jnp.where(lane < members - room, moved, pltpu.roll(third, members - room, 1))
        return jnp.concatenate([first, last], axis=1), lane, room

    def state_wide(value):
        return widen(value, True)[0].astype(BF16)

    def prior_wide(value):
        wide, lane, room = widen(jnp.where(lane_ids(value.shape) < members, value, 0.0), False)
        wide_lane = lane_ids(wide.shape)
        return jnp.where(wide_lane < 3 * members, wide, 0.0).astype(BF16)

    def lon_weight(gap):
        gap = jnp.abs(gap)
        gap = jnp.minimum(gap, lon_total - gap)
        return jnp.maximum(0.0, 1.0 - gap * (1.0 / span))

    def lat_weight(gap):
        return 1.0 - jnp.abs(gap) * (1.0 / lat_total)

    def obs_taper(rows, s):
        lat, lon = rows[:, members + 1:members + 2], rows[:, members + 2:members + 3]
        return lat_weight(lat - lat_ref[s]) * lon_weight(lon - lon_ref[s])

    def apply(rows, high, low):
        both = nn(high, vw_s[...])
        return rows - (both[:, :LANES] + both[:, LANES:] + nn(low, vw_s[:, :LANES]))

    def update(rows, taper, s):
        gained = nt(state_wide(rows), z3_s[lax.rem(s, 2)]) * taper
        return apply(rows, *split(gained))

    def update_cells(source_ref, s):
        def some(i, _):
            tapers = []
            for k in range(chunk):
                c = i * chunk + k
                lat = (band * lat_dev + lax.rem(c, lat_dev)).astype(F32)
                lon = (column * lon_dev + c // lat_dev).astype(F32)
                weight = lat_weight(lat - lat_ref[s]) * lon_weight(lon - lon_ref[s])
                tapers.append(jnp.broadcast_to(weight, (levels, obs)))
            here = pl.ds(pl.multiple_of(i * (chunk * levels), chunk * levels), chunk * levels)
            cells_s[here, :] = update(source_ref[here, :], jnp.concatenate(tapers, axis=0), s)
            return 0

        lax.fori_loop(0, classes // chunk, some, 0)

    def at(t):
        return pl.ds(pl.multiple_of(t * obs, obs), obs)

    cells_s[...] = state_ref[...]
    obs_s[...] = obs_ref[...]

    def turn(t, _):
        prior = obs_s[at(t), :]
        lane = lane_ids(prior.shape)
        innovation = pltpu.roll(prior, LANES - 3, 1) - prior
        joined = jnp.where(lane < members, prior, jnp.where(lane == members, innovation, 0.0))
        high, low = split(joined)
        batch_id = order_ref[t]
        table_high, table_low = split(jnp.concatenate([root_ref[batch_id], gain_ref[batch_id]], axis=0))
        both = nn(table_high, jnp.concatenate([high, low], axis=1))
        part = both[:, :LANES] + both[:, LANES:] + nn(table_low, high)
        lane = lane_ids((quarter, LANES))
        weighted = jnp.where(lane < members, part[:quarter], jnp.where(lane == members, -part[quarter:], 0.0))
        mine = pl.ds(pl.multiple_of(band * quarter, quarter), quarter)
        v_s[t, mine, :] = weighted * (1.0 / (members - 1.0))

        def copy(k):
            return pltpu.make_async_remote_copy(
                src_ref=v_s.at[t, mine, :],
                dst_ref=v_s.at[t, mine, :],
                send_sem=send_sem.at[t, k - 1],
                recv_sem=recv_sem.at[t, k - 1],
                device_id={"gy": lax.rem(band + k, bands)},
                device_id_type=MESH,
            )

        for k in range(1, bands):
            copy(k).start()

        z3_s[lax.rem(t, 2)] = prior_wide(prior)

        @pl.when(t < batches - 1)
        def _():
            rows = obs_s[at(t + 1), :]

            @pl.when(t > 0)
            def _():
                obs_s[at(t + 1), :] = update(rows, obs_taper(rows, t - 1), t - 1)

            rows = obs_s[at(t + 1), :]
            gained = nt(state_wide(rows), z3_s[lax.rem(t, 2)]) * obs_taper(rows, t)
            gh_s[...], gl_s[...] = split(gained)

        @pl.when(t > 0)
        def _():
            def later(n, _):
                rows = obs_s[at(n), :]
                obs_s[at(n), :] = update(rows, obs_taper(rows, t - 1), t - 1)
                return 0

            lax.fori_loop(t + 2, batches, later, 0)
            update_cells(cells_s, t - 1)

        for k in range(1, bands):
            copy(k).wait()

        vw_s[...] = jnp.concatenate(split(v_s[t]), axis=1)

        @pl.when(t < batches - 1)
        def _():
            obs_s[at(t + 1), :] = apply(obs_s[at(t + 1), :], gh_s[...], gl_s[...])

        return 0

    lax.fori_loop(0, batches, turn, 0)
    update_cells(cells_s, batches - 1)
    for c in range(classes):
        tall = cells_s[pl.ds(c * levels, levels), :].T
        anom_out[:, c, :] = tall[:members]
        mean_out[pl.ds(c, 1), :] = tall[members:members + 1]


def local(anomalies, state_mean, obs_value, obs_cell, owner, order, root_inv, gain_inv):
    members, lon_dev, lat_dev, levels = anomalies.shape
    classes = lon_dev * lat_dev
    cells = classes * levels
    batches, quarter = obs_value.shape
    obs = obs_cell.shape[1]
    slabs, bands = lax.axis_size("gx"), lax.axis_size("gy")
    band = lax.axis_index("gy")
    owned = owner[order]
    cells_of = obs_cell[order]
    own_cells = lax.dynamic_slice_in_dim(cells_of, band * quarter, quarter, axis=1)
    own_values = obs_value[order]
    obs_lat = jnp.arange(obs, dtype=jnp.int32)[None, :] // quarter * lat_dev + cells_of // levels % lat_dev
    obs_lon = owned[:, None] * lon_dev + cells_of // (lat_dev * levels)

    state, rows = pl.pallas_call(
        functools.partial(pick_kernel, lon_dev, lat_dev),
        out_shape=(
            jax.ShapeDtypeStruct((cells, LANES), F32),
            jax.ShapeDtypeStruct((batches * quarter, LANES), F32),
        ),
        in_specs=[SMEM, SMEM, SMEM, VMEM, VMEM],
        out_specs=(VMEM, VMEM),
        name="pick",
    )(own_cells, own_values, owned, anomalies.reshape(members, classes, levels), state_mean.reshape(classes, levels))

    rows = lax.psum(rows.reshape(batches, quarter, LANES), "gx")
    rows = lax.all_gather(rows, "gy", axis=1, tiled=True).reshape(batches * obs, LANES)

    sizes = (
        members, lon_dev, lat_dev, levels, float(slabs * lon_dev), float(bands * lat_dev), REACH * lon_dev + 1.0, bands
    )
    post, mean = pl.pallas_call(
        functools.partial(main_kernel, sizes),
        out_shape=(
            jax.ShapeDtypeStruct((members, classes, levels), F32),
            jax.ShapeDtypeStruct((classes, levels), F32),
        ),
        in_specs=[SMEM] + [VMEM] * 6,
        out_specs=(VMEM, VMEM),
        scratch_shapes=[
            pltpu.VMEM((cells, LANES), F32),
            pltpu.VMEM((batches * obs, LANES), F32),
            pltpu.VMEM((batches, obs, LANES), F32),
            pltpu.VMEM((obs, 2 * LANES), BF16),
            pltpu.VMEM((2, obs, 2 * LANES), BF16),
            pltpu.VMEM((obs, obs), BF16),
            pltpu.VMEM((obs, obs), BF16),
            pltpu.SemaphoreType.DMA((batches, bands - 1)),
            pltpu.SemaphoreType.DMA((batches, bands - 1)),
        ],
        compiler_params=pltpu.CompilerParams(collective_id=0, has_side_effects=True),
        name="analysis",
    )(
        order, state, rows, obs_lat.astype(F32)[:, None, :], obs_lon.astype(F32)[:, None, :], root_inv, gain_inv,
    )
    return post.reshape(members, lon_dev, lat_dev, levels), mean.reshape(lon_dev, lat_dev, levels)


def solution(mesh):
    return jax.shard_map(
        local,
        mesh=mesh,
        in_specs=(
            P(None, "gx", "gy", None),
            P("gx", "gy", None),
            P(None, "gy"),
            P(),
            P(),
            P(),
            P(None, "gy", None),
            P(None, "gy", None),
        ),
        out_specs=(P(None, "gx", "gy", None), P("gx", "gy", None)),
        check_vma=False,
    )
```

```python
import functools

import jax
import jax.numpy as jnp
from jax import lax
from jax.experimental import pallas as pl
from jax.experimental.pallas import tpu as pltpu
from jax.sharding import PartitionSpec as P

REACH = 3
LANES = 128
MESH = pl.DeviceIdType.MESH
VMEM = pl.BlockSpec(memory_space=pltpu.VMEM)
SMEM = pl.BlockSpec(memory_space=pltpu.SMEM)
F32 = jnp.float32
BF16 = jnp.bfloat16


def split(value):
    high = value.astype(BF16)
    return high, (value - high.astype(F32)).astype(BF16)


def nn(left, right):
    return lax.dot_general(left, right, (((1,), (0,)), ((), ())), preferred_element_type=F32)


def nt(left, right):
    return lax.dot_general(left, right, (((1,), (1,)), ((), ())), preferred_element_type=F32)


def lane_ids(shape):
    return lax.broadcasted_iota(jnp.int32, shape, len(shape) - 1)


def pick_kernel(lon_dev, lat_dev, cells_ref, value_ref, owner_ref, order_ref, anom_ref, mean_ref, state_ref, rows_ref):
    column, band = lax.axis_index("gx"), lax.axis_index("gy")
    members, classes, levels = anom_ref.shape
    batches, quarter = value_ref.shape

    for c in range(classes):
        lat = (band * lat_dev + c % lat_dev).astype(F32)
        lon = (column * lon_dev + c // lat_dev).astype(F32)
        tall = jnp.concatenate(
            [
                anom_ref[:, c, :],
                mean_ref[pl.ds(c, 1), :],
                jnp.full((1, levels), lat, F32),
                jnp.full((1, levels), lon, F32),
                jnp.zeros((LANES - members - 3, levels), F32),
            ],
            axis=0,
        )
        state_ref[pl.ds(c * levels, levels), :] = tall.T

    lane = lane_ids((1, LANES))

    def batch(t, _):
        b = order_ref[t]
        mine = owner_ref[b] == column

        @pl.when(mine)
        def _():
            def group(i, _):
                for k in range(8):
                    j = i * 8 + k
                    row = state_ref[pl.ds(cells_ref[b, band * quarter + j], 1), :]
                    rows_ref[pl.ds(t * quarter + j, 1), :] = jnp.where(lane == members + 3, value_ref[b, j], row)
                return 0

            lax.fori_loop(0, quarter // 8, group, 0)

        @pl.when(jnp.logical_not(mine))
        def _():
            rows_ref[pl.ds(pl.multiple_of(t * quarter, quarter), quarter), :] = jnp.zeros((quarter, LANES), F32)

        return 0

    lax.fori_loop(0, batches, batch, 0)


def spread_kernel(bands, slabs, rows_ref, out_ref, land, send1, recv1, send2, recv2, send3, recv3, send4, recv4, send5, recv5):
    x, b = lax.axis_index("gx"), lax.axis_index("gy")
    partner = b + 1 - 2 * lax.rem(b, 2)
    across = lax.rem(b + 2, bands)
    chunk = land.shape[1]

    def piece(q):
        return pl.ds(pl.multiple_of(q * chunk, chunk), chunk)

    def slab(k):
        return lax.rem(x + k, slabs)

    def source(k):
        return lax.rem(x + slabs - k, slabs)

    def first(k):
        return pltpu.make_async_remote_copy(
            src_ref=rows_ref.at[piece(slab(k)), :], dst_ref=land.at[k], send_sem=send1.at[k], recv_sem=recv1.at[k],
            device_id={"gx": slab(k)}, device_id_type=MESH,
        )

    def second(k):
        return pltpu.make_async_remote_copy(
            src_ref=out_ref.at[b, piece(x), :], dst_ref=out_ref.at[b, piece(x), :], send_sem=send2.at[k],
            recv_sem=recv2.at[k], device_id={"gx": slab(k)}, device_id_type=MESH,
        )

    def hand(k, of_band, send_sem, recv_sem, target):
        place = out_ref.at[of_band, piece(source(k)), :]
        return pltpu.make_async_remote_copy(
            src_ref=place, dst_ref=place, send_sem=send_sem.at[k], recv_sem=recv_sem.at[k],
            device_id={"gy": target}, device_id_type=MESH,
        )

    def third(k):
        return hand(k, b, send3, recv3, partner)

    def fourth(k):
        return hand(k, b, send4, recv4, across)

    def fifth(k):
        return hand(k, across, send5, recv5, partner)

    def each(low, high, body):
        def step(k, _):
            body(k)
            return 0

        lax.fori_loop(low, high, step, 0)

    barrier = pltpu.get_barrier_semaphore()
    each(1, slabs, lambda k: pl.semaphore_signal(barrier, inc=1, device_id={"gx": slab(k)}, device_id_type=MESH))
    for target in (partner, across):
        pl.semaphore_signal(barrier, inc=1, device_id={"gy": target}, device_id_type=MESH)
    pl.semaphore_wait(barrier, slabs + 1)

    each(1, slabs, lambda k: first(k).start())
    out_ref[b, piece(x), :] = rows_ref[piece(x), :]

    def add(k):
        first(k).wait_recv()
        out_ref[b, piece(x), :] += land[k]

    each(1, slabs, add)
    fourth(0).start()
    each(1, slabs, lambda k: second(k).start())
    third(0).start()

    def relay(k):
        second(k).wait_recv()
        fourth(k).start()
        third(k).start()
        fourth(k - 1).wait_recv()
        fifth(k - 1).start()

    each(1, slabs, relay)
    fourth(slabs - 1).wait_recv()
    fifth(slabs - 1).start()

    def finish(k):
        third(k).wait()
        fifth(k).wait()
        fourth(k).wait_send()

    each(0, slabs, finish)

    def sent(k):
        first(k).wait_send()
        second(k).wait_send()

    each(1, slabs, sent)


def main_kernel(
    sizes, order_ref, owner_ref, state_ref, obs_ref, cell_ref, root_ref, gain_ref,
    anom_out, mean_out,
    lat_ref, lon_ref, cells_s, obs_s, v_s, vw_s, z3_s, gh_s, gl_s, send_sem, recv_sem,
):
    members, lon_dev, lat_dev, levels, lon_total, lat_total, span, bands = sizes
    batches, obs = cell_ref.shape
    quarter = obs // bands
    column, band = lax.axis_index("gx"), lax.axis_index("gy")
    classes = lon_dev * lat_dev
    chunk = 4

    barrier = pltpu.get_barrier_semaphore()
    for k in range(1, bands):
        pl.semaphore_signal(barrier, inc=1, device_id={"gy": lax.rem(band + k, bands)}, device_id_type=MESH)
    pl.semaphore_wait(barrier, bands - 1)

    def widen(value, with_low_in_middle):
        high, low = split(value)
        high, low = high.astype(F32), low.astype(F32)
        second, third = (low, high) if with_low_in_middle else (high, low)
        lane = lane_ids(value.shape)
        room = LANES - members
        moved = pltpu.roll(second, members, 1)
        first = jnp.where(lane < members, high, moved)
        last = jnp.where(lane < members - room, moved, pltpu.roll(third, members - room, 1))
        return jnp.concatenate([first, last], axis=1), lane, room

    def state_wide(value):
        return widen(value, True)[0].astype(BF16)

    def prior_wide(value):
        wide, lane, room = widen(jnp.where(lane_ids(value.shape) < members, value, 0.0), False)
        wide_lane = lane_ids(wide.shape)
        return jnp.where(wide_lane < 3 * members, wide, 0.0).astype(BF16)

    def lon_weight(gap):
        gap = jnp.abs(gap)
        gap = jnp.minimum(gap, lon_total - gap)
        return jnp.maximum(0.0, 1.0 - gap * (1.0 / span))

    def lat_weight(gap):
        return 1.0 - jnp.abs(gap) * (1.0 / lat_total)

    def obs_taper(rows, s):
        lat, lon = rows[:, members + 1:members + 2], rows[:, members + 2:members + 3]
        return lat_weight(lat - lat_ref[s]) * lon_weight(lon - lon_ref[s])

    def apply(rows, high, low):
        both = nn(high, vw_s[...])
        return rows - (both[:, :LANES] + both[:, LANES:] + nn(low, vw_s[:, :LANES]))

    def update(rows, taper, s, slot):
        gained = nt(state_wide(rows), z3_s[slot]) * taper
        return apply(rows, *split(gained))

    def update_cells(s, slot):
        for i in range(classes // chunk):
            tapers = []
            for k in range(chunk):
                c = i * chunk + k
                lat = (band * lat_dev + c % lat_dev).astype(F32)
                lon = (column * lon_dev + c // lat_dev).astype(F32)
                weight = lat_weight(lat - lat_ref[s]) * lon_weight(lon - lon_ref[s])
                tapers.append(jnp.broadcast_to(weight, (levels, obs)))
            here = pl.ds(i * chunk * levels, chunk * levels)
            cells_s[here, :] = update(cells_s[here, :], jnp.concatenate(tapers, axis=0), s, slot)

    def at(t):
        return pl.ds(pl.multiple_of(t * obs, obs), obs)

    cells_s[...] = state_ref[...]
    for t in range(batches):
        for q in range(bands):
            obs_s[pl.ds(t * obs + q * quarter, quarter), :] = obs_ref[q, pl.ds(t * quarter, quarter), :]
    obs_s[pl.ds(batches * obs, 2 * obs), :] = jnp.zeros((2 * obs, LANES), F32)
    vw_s[...] = jnp.zeros_like(vw_s)
    z3_s[...] = jnp.zeros_like(z3_s)
    first_lat = lax.broadcasted_iota(jnp.int32, (1, obs), 1).astype(F32)
    first_lat = jnp.floor((first_lat + 0.5) * (1.0 / quarter)) * lat_dev
    for t in range(batches):
        batch_id = order_ref[t]
        level_row = jnp.floor((cell_ref[pl.ds(batch_id, 1), :].astype(F32) + 0.5) * (1.0 / levels))
        lon_row = jnp.floor((level_row + 0.5) * (1.0 / lat_dev))
        lat_ref[t] = level_row - lon_row * lat_dev + first_lat
        lon_ref[t] = lon_row + (owner_ref[batch_id] * lon_dev).astype(F32)

    def turn(t, _):
        prior = obs_s[at(t), :]
        lane = lane_ids(prior.shape)
        innovation = pltpu.roll(prior, LANES - 3, 1) - prior
        joined = jnp.where(lane < members, prior, jnp.where(lane == members, innovation, 0.0))
        high, low = split(joined)
        batch_id = order_ref[t]
        table_high, table_low = split(jnp.concatenate([root_ref[batch_id], gain_ref[batch_id]], axis=0))
        both = nn(table_high, jnp.concatenate([high, low], axis=1))
        part = both[:, :LANES] + both[:, LANES:] + nn(table_low, high)
        lane = lane_ids((quarter, LANES))
        weighted = jnp.where(lane < members, part[:quarter], jnp.where(lane == members, -part[quarter:], 0.0))
        mine = pl.ds(pl.multiple_of(band * quarter, quarter), quarter)
        v_s[t, mine, :] = weighted * (1.0 / (members - 1.0))

        def copy(k):
            return pltpu.make_async_remote_copy(
                src_ref=v_s.at[t, mine, :],
                dst_ref=v_s.at[t, mine, :],
                send_sem=send_sem.at[t, k - 1],
                recv_sem=recv_sem.at[t, k - 1],
                device_id={"gy": lax.rem(band + k, bands)},
                device_id_type=MESH,
            )

        for k in range(1, bands):
            copy(k).start()

        z3_s[lax.rem(t, 2)] = prior_wide(prior)

        before = jnp.maximum(t - 1, 0)
        past = lax.rem(t + 1, 2)
        rows = obs_s[at(t + 1), :]
        rows = update(rows, obs_taper(rows, before), before, past)
        obs_s[at(t + 1), :] = rows
        gained = nt(state_wide(rows), z3_s[lax.rem(t, 2)]) * obs_taper(rows, t)
        gh_s[...], gl_s[...] = split(gained)
        update_cells(before, past)

        def later(i, _):
            here = pl.ds(pl.multiple_of((t + 2 + 2 * i) * obs, obs), 2 * obs)
            rows = obs_s[here, :]
            obs_s[here, :] = update(rows, obs_taper(rows, before), before, past)
            return 0

        lax.fori_loop(0, (batches - 1 - t) // 2 * jnp.minimum(t, 1), later, 0)

        for k in range(1, bands):
            copy(k).wait()

        vw_s[...] = jnp.concatenate(split(v_s[t]), axis=1)

        obs_s[at(t + 1), :] = apply(obs_s[at(t + 1), :], gh_s[...], gl_s[...])
        return 0

    lax.fori_loop(0, batches, turn, 0)
    update_cells(batches - 1, (batches - 1) % 2)
    for c in range(classes):
        tall = cells_s[pl.ds(c * levels, levels), :].T
        anom_out[:, c, :] = tall[:members]
        mean_out[pl.ds(c, 1), :] = tall[members:members + 1]


def local(anomalies, state_mean, obs_value, obs_cell, owner, order, root_inv, gain_inv):
    members, lon_dev, lat_dev, levels = anomalies.shape
    classes = lon_dev * lat_dev
    cells = classes * levels
    batches, quarter = obs_value.shape
    obs = obs_cell.shape[1]
    slabs, bands = lax.axis_size("gx"), lax.axis_size("gy")
    state, rows = pl.pallas_call(
        functools.partial(pick_kernel, lon_dev, lat_dev),
        out_shape=(
            jax.ShapeDtypeStruct((cells, LANES), F32),
            jax.ShapeDtypeStruct((batches * quarter, LANES), F32),
        ),
        in_specs=[SMEM] * 4 + [VMEM] * 2,
        out_specs=(VMEM, VMEM),
        name="pick",
    )(
        obs_cell, obs_value, owner, order,
        anomalies.reshape(members, classes, levels), state_mean.reshape(classes, levels),
    )

    chunk = batches * quarter // slabs
    rows = pl.pallas_call(
        functools.partial(spread_kernel, bands, slabs),
        out_shape=jax.ShapeDtypeStruct((bands, batches * quarter, LANES), F32),
        in_specs=[VMEM],
        out_specs=VMEM,
        scratch_shapes=[pltpu.VMEM((slabs, chunk, LANES), F32)] + [pltpu.SemaphoreType.DMA((slabs,))] * 10,
        compiler_params=pltpu.CompilerParams(collective_id=1, has_side_effects=True),
        name="spread",
    )(rows)

    sizes = (
        members, lon_dev, lat_dev, levels, float(slabs * lon_dev), float(bands * lat_dev), REACH * lon_dev + 1.0, bands
    )
    post, mean = pl.pallas_call(
        functools.partial(main_kernel, sizes),
        out_shape=(
            jax.ShapeDtypeStruct((members, classes, levels), F32),
            jax.ShapeDtypeStruct((classes, levels), F32),
        ),
        in_specs=[SMEM] * 2 + [VMEM] * 5,
        out_specs=(VMEM, VMEM),
        scratch_shapes=[
            pltpu.VMEM((batches, 1, obs), F32),
            pltpu.VMEM((batches, 1, obs), F32),
            pltpu.VMEM((cells, LANES), F32),
            pltpu.VMEM(((batches + 2) * obs, LANES), F32),
            pltpu.VMEM((batches, obs, LANES), F32),
            pltpu.VMEM((obs, 2 * LANES), BF16),
            pltpu.VMEM((2, obs, 2 * LANES), BF16),
            pltpu.VMEM((obs, obs), BF16),
            pltpu.VMEM((obs, obs), BF16),
            pltpu.SemaphoreType.DMA((batches, bands - 1)),
            pltpu.SemaphoreType.DMA((batches, bands - 1)),
        ],
        compiler_params=pltpu.CompilerParams(collective_id=0, has_side_effects=True),
        name="analysis",
    )(
        order, owner, state, rows, obs_cell, root_inv, gain_inv,
    )
    return post.reshape(members, lon_dev, lat_dev, levels), mean.reshape(lon_dev, lat_dev, levels)


def solution(mesh):
    return jax.shard_map(
        local,
        mesh=mesh,
        in_specs=(
            P(None, "gx", "gy", None),
            P("gx", "gy", None),
            P(None, "gy"),
            P(),
            P(),
            P(),
            P(None, "gy", None),
            P(None, "gy", None),
        ),
        out_specs=(P(None, "gx", "gy", None), P("gx", "gy", None)),
        check_vma=False,
    )
```

```python
import functools

import jax
import jax.numpy as jnp
from jax import lax
from jax.experimental import pallas as pl
from jax.experimental.pallas import tpu as pltpu
from jax.sharding import PartitionSpec as P

REACH = 3
LANES = 128
MESH = pl.DeviceIdType.MESH
VMEM = pl.BlockSpec(memory_space=pltpu.VMEM)
SMEM = pl.BlockSpec(memory_space=pltpu.SMEM)
F32 = jnp.float32
BF16 = jnp.bfloat16


def split(value):
    high = value.astype(BF16)
    return high, (value - high.astype(F32)).astype(BF16)


def nn(left, right):
    return lax.dot_general(left, right, (((1,), (0,)), ((), ())), preferred_element_type=F32)


def nt(left, right):
    return lax.dot_general(left, right, (((1,), (1,)), ((), ())), preferred_element_type=F32)


def lane_ids(shape):
    return lax.broadcasted_iota(jnp.int32, shape, len(shape) - 1)


def pick_kernel(lon_dev, lat_dev, cells_ref, value_ref, owner_ref, order_ref, anom_ref, mean_ref, state_ref, packed_ref, rows_ref):
    column, band = lax.axis_index("gx"), lax.axis_index("gy")
    members, classes, levels = anom_ref.shape
    batches, quarter = value_ref.shape

    for c in range(classes):
        lat = (band * lat_dev + c % lat_dev).astype(F32)
        lon = (column * lon_dev + c // lat_dev).astype(F32)
        tall = jnp.concatenate(
            [
                anom_ref[:, c, :],
                mean_ref[pl.ds(c, 1), :],
                jnp.full((1, levels), lat, F32),
                jnp.full((1, levels), lon, F32),
                jnp.zeros((LANES - members - 3, levels), F32),
            ],
            axis=0,
        )
        state_ref[pl.ds(c * levels, levels), :] = tall.T

    lane = lane_ids((1, LANES))

    def batch(t, _):
        b = order_ref[t]
        mine = owner_ref[b] == column

        @pl.when(mine)
        def _():
            def group(i, _):
                for k in range(8):
                    j = i * 8 + k
                    row = state_ref[pl.ds(cells_ref[b, band * quarter + j], 1), :]
                    rows_ref[pl.ds(t * quarter + j, 1), :] = jnp.where(lane == members + 3, value_ref[b, j], row)
                return 0

            lax.fori_loop(0, quarter // 8, group, 0)

        @pl.when(jnp.logical_not(mine))
        def _():
            rows_ref[pl.ds(pl.multiple_of(t * quarter, quarter), quarter), :] = jnp.zeros((quarter, LANES), F32)

        return 0

    lax.fori_loop(0, batches, batch, 0)
    slabs, height, chunk = packed_ref.shape
    for q in range(slabs):
        packed_ref[q] = rows_ref[pl.ds(q * chunk, chunk), :].T[:height]


def spread_kernel(bands, slabs, rows_ref, out_ref, land, send1, recv1, send2, recv2, send3, recv3, send4, recv4, send5, recv5):
    x, b = lax.axis_index("gx"), lax.axis_index("gy")
    partner = b + 1 - 2 * lax.rem(b, 2)
    across = lax.rem(b + 2, bands)

    def slab(k):
        return lax.rem(x + k, slabs)

    def source(k):
        return lax.rem(x + slabs - k, slabs)

    def first(k):
        return pltpu.make_async_remote_copy(
            src_ref=rows_ref.at[slab(k)], dst_ref=land.at[k], send_sem=send1.at[k], recv_sem=recv1.at[k],
            device_id={"gx": slab(k)}, device_id_type=MESH,
        )

    def second(k):
        return pltpu.make_async_remote_copy(
            src_ref=out_ref.at[b, x], dst_ref=out_ref.at[b, x], send_sem=send2.at[k],
            recv_sem=recv2.at[k], device_id={"gx": slab(k)}, device_id_type=MESH,
        )

    def hand(k, of_band, send_sem, recv_sem, target):
        place = out_ref.at[of_band, source(k)]
        return pltpu.make_async_remote_copy(
            src_ref=place, dst_ref=place, send_sem=send_sem.at[k], recv_sem=recv_sem.at[k],
            device_id={"gy": target}, device_id_type=MESH,
        )

    def third(k):
        return hand(k, b, send3, recv3, partner)

    def fourth(k):
        return hand(k, b, send4, recv4, across)

    def fifth(k):
        return hand(k, across, send5, recv5, partner)

    def each(low, high, body):
        def step(k, _):
            body(k)
            return 0

        lax.fori_loop(low, high, step, 0)

    barrier = pltpu.get_barrier_semaphore()
    each(1, slabs, lambda k: pl.semaphore_signal(barrier, inc=1, device_id={"gx": slab(k)}, device_id_type=MESH))
    for target in (partner, across):
        pl.semaphore_signal(barrier, inc=1, device_id={"gy": target}, device_id_type=MESH)
    pl.semaphore_wait(barrier, slabs + 1)

    each(1, slabs, lambda k: first(k).start())
    out_ref[b, x] = rows_ref[x]

    def add(k):
        first(k).wait_recv()
        out_ref[b, x] += land[k]

    each(1, slabs, add)
    fourth(0).start()
    each(1, slabs, lambda k: second(k).start())
    third(0).start()

    def relay(k):
        second(k).wait_recv()
        fourth(k).start()
        third(k).start()
        fourth(k - 1).wait_recv()
        fifth(k - 1).start()

    each(1, slabs, relay)
    fourth(slabs - 1).wait_recv()
    fifth(slabs - 1).start()

    def finish(k):
        third(k).wait()
        fifth(k).wait()
        fourth(k).wait_send()

    each(0, slabs, finish)

    def sent(k):
        first(k).wait_send()
        second(k).wait_send()

    each(1, slabs, sent)


def main_kernel(
    sizes, order_ref, owner_ref, state_ref, obs_ref, cell_ref, root_ref, gain_ref,
    anom_out, mean_out,
    lat_ref, lon_ref, cells_s, obs_s, v_s, vw_s, z3_s, gh_s, gl_s, send_sem, recv_sem,
):
    members, lon_dev, lat_dev, levels, lon_total, lat_total, span, bands = sizes
    batches, obs = cell_ref.shape
    quarter = obs // bands
    column, band = lax.axis_index("gx"), lax.axis_index("gy")
    classes = lon_dev * lat_dev
    chunk = 4

    barrier = pltpu.get_barrier_semaphore()
    for k in range(1, bands):
        pl.semaphore_signal(barrier, inc=1, device_id={"gy": lax.rem(band + k, bands)}, device_id_type=MESH)
    pl.semaphore_wait(barrier, bands - 1)

    def widen(value, with_low_in_middle):
        high, low = split(value)
        high, low = high.astype(F32), low.astype(F32)
        second, third = (low, high) if with_low_in_middle else (high, low)
        lane = lane_ids(value.shape)
        room = LANES - members
        moved = pltpu.roll(second, members, 1)
        first = jnp.where(lane < members, high, moved)
        last = jnp.where(lane < members - room, moved, pltpu.roll(third, members - room, 1))
        return jnp.concatenate([first, last], axis=1), lane, room

    def state_wide(value):
        return widen(value, True)[0].astype(BF16)

    def prior_wide(value):
        wide, lane, room = widen(jnp.where(lane_ids(value.shape) < members, value, 0.0), False)
        wide_lane = lane_ids(wide.shape)
        return jnp.where(wide_lane < 3 * members, wide, 0.0).astype(BF16)

    def lon_weight(gap):
        gap = jnp.abs(gap)
        gap = jnp.minimum(gap, lon_total - gap)
        return jnp.maximum(0.0, 1.0 - gap * (1.0 / span))

    def lat_weight(gap):
        return 1.0 - jnp.abs(gap) * (1.0 / lat_total)

    def obs_taper(rows, s):
        lat, lon = rows[:, members + 1:members + 2], rows[:, members + 2:members + 3]
        return lat_weight(lat - lat_ref[s]) * lon_weight(lon - lon_ref[s])

    def apply(rows, high, low):
        both = nn(high, vw_s[...])
        return rows - (both[:, :LANES] + both[:, LANES:] + nn(low, vw_s[:, :LANES]))

    def update(rows, taper, s, slot):
        gained = nt(state_wide(rows), z3_s[slot]) * taper
        return apply(rows, *split(gained))

    def update_cells(s, slot):
        for i in range(classes // chunk):
            tapers = []
            for k in range(chunk):
                c = i * chunk + k
                lat = (band * lat_dev + c % lat_dev).astype(F32)
                lon = (column * lon_dev + c // lat_dev).astype(F32)
                weight = lat_weight(lat - lat_ref[s]) * lon_weight(lon - lon_ref[s])
                tapers.append(jnp.broadcast_to(weight, (levels, obs)))
            here = pl.ds(i * chunk * levels, chunk * levels)
            cells_s[here, :] = update(cells_s[here, :], jnp.concatenate(tapers, axis=0), s, slot)

    def at(t):
        return pl.ds(pl.multiple_of(t * obs, obs), obs)

    cells_s[...] = state_ref[...]
    _, slabs, height, width = obs_ref.shape
    part = min(width, quarter)
    for q in range(bands):
        for p in range(slabs):
            rest = jnp.zeros((LANES - height, width), F32)
            block = jnp.concatenate([obs_ref[q, p], rest], axis=0).T
            for i in range(0, width, part):
                t, j = divmod(p * width + i, quarter)
                obs_s[pl.ds(t * obs + q * quarter + j, part), :] = block[i:i + part]
    obs_s[pl.ds(batches * obs, 2 * obs), :] = jnp.zeros((2 * obs, LANES), F32)
    vw_s[...] = jnp.zeros_like(vw_s)
    z3_s[...] = jnp.zeros_like(z3_s)
    first_lat = lax.broadcasted_iota(jnp.int32, (1, obs), 1).astype(F32)
    first_lat = jnp.floor((first_lat + 0.5) * (1.0 / quarter)) * lat_dev
    for t in range(batches):
        batch_id = order_ref[t]
        level_row = jnp.floor((cell_ref[pl.ds(batch_id, 1), :].astype(F32) + 0.5) * (1.0 / levels))
        lon_row = jnp.floor((level_row + 0.5) * (1.0 / lat_dev))
        lat_ref[t] = level_row - lon_row * lat_dev + first_lat
        lon_ref[t] = lon_row + (owner_ref[batch_id] * lon_dev).astype(F32)

    def turn(t, _):
        prior = obs_s[at(t), :]
        lane = lane_ids(prior.shape)
        innovation = pltpu.roll(prior, LANES - 3, 1) - prior
        joined = jnp.where(lane < members, prior, jnp.where(lane == members, innovation, 0.0))
        high, low = split(joined)
        batch_id = order_ref[t]
        table_high, table_low = split(jnp.concatenate([root_ref[batch_id], gain_ref[batch_id]], axis=0))
        both = nn(table_high, jnp.concatenate([high, low], axis=1))
        part = both[:, :LANES] + both[:, LANES:] + nn(table_low, high)
        lane = lane_ids((quarter, LANES))
        weighted = jnp.where(lane < members, part[:quarter], jnp.where(lane == members, -part[quarter:], 0.0))
        mine = pl.ds(pl.multiple_of(band * quarter, quarter), quarter)
        v_s[t, mine, :] = weighted * (1.0 / (members - 1.0))

        def copy(k):
            return pltpu.make_async_remote_copy(
                src_ref=v_s.at[t, mine, :],
                dst_ref=v_s.at[t, mine, :],
                send_sem=send_sem.at[t, k - 1],
                recv_sem=recv_sem.at[t, k - 1],
                device_id={"gy": lax.rem(band + k, bands)},
                device_id_type=MESH,
            )

        for k in range(1, bands):
            copy(k).start()

        z3_s[lax.rem(t, 2)] = prior_wide(prior)

        before = jnp.maximum(t - 1, 0)
        past = lax.rem(t + 1, 2)
        rows = obs_s[at(t + 1), :]
        rows = update(rows, obs_taper(rows, before), before, past)
        obs_s[at(t + 1), :] = rows
        gained = nt(state_wide(rows), z3_s[lax.rem(t, 2)]) * obs_taper(rows, t)
        gh_s[...], gl_s[...] = split(gained)
        update_cells(before, past)

        def later(i, _):
            here = pl.ds(pl.multiple_of((t + 2 + 2 * i) * obs, obs), 2 * obs)
            rows = obs_s[here, :]
            obs_s[here, :] = update(rows, obs_taper(rows, before), before, past)
            return 0

        lax.fori_loop(0, (batches - 1 - t) // 2 * jnp.minimum(t, 1), later, 0)

        for k in range(1, bands):
            copy(k).wait()

        vw_s[...] = jnp.concatenate(split(v_s[t]), axis=1)

        obs_s[at(t + 1), :] = apply(obs_s[at(t + 1), :], gh_s[...], gl_s[...])
        return 0

    lax.fori_loop(0, batches, turn, 0)
    update_cells(batches - 1, (batches - 1) % 2)
    for c in range(classes):
        tall = cells_s[pl.ds(c * levels, levels), :].T
        anom_out[:, c, :] = tall[:members]
        mean_out[pl.ds(c, 1), :] = tall[members:members + 1]


def local(anomalies, state_mean, obs_value, obs_cell, owner, order, root_inv, gain_inv):
    members, lon_dev, lat_dev, levels = anomalies.shape
    classes = lon_dev * lat_dev
    cells = classes * levels
    batches, quarter = obs_value.shape
    obs = obs_cell.shape[1]
    slabs, bands = lax.axis_size("gx"), lax.axis_size("gy")
    chunk = batches * quarter // slabs
    height = (members + 4 + 7) // 8 * 8
    state, rows = pl.pallas_call(
        functools.partial(pick_kernel, lon_dev, lat_dev),
        out_shape=(
            jax.ShapeDtypeStruct((cells, LANES), F32),
            jax.ShapeDtypeStruct((slabs, height, chunk), F32),
        ),
        in_specs=[SMEM] * 4 + [VMEM] * 2,
        out_specs=(VMEM, VMEM),
        scratch_shapes=[pltpu.VMEM((batches * quarter, LANES), F32)],
        name="pick",
    )(
        obs_cell, obs_value, owner, order,
        anomalies.reshape(members, classes, levels), state_mean.reshape(classes, levels),
    )

    rows = pl.pallas_call(
        functools.partial(spread_kernel, bands, slabs),
        out_shape=jax.ShapeDtypeStruct((bands, slabs, height, chunk), F32),
        in_specs=[VMEM],
        out_specs=VMEM,
        scratch_shapes=[pltpu.VMEM((slabs, height, chunk), F32)] + [pltpu.SemaphoreType.DMA((slabs,))] * 10,
        compiler_params=pltpu.CompilerParams(collective_id=1, has_side_effects=True),
        name="spread",
    )(rows)

    sizes = (
        members, lon_dev, lat_dev, levels, float(slabs * lon_dev), float(bands * lat_dev), REACH * lon_dev + 1.0, bands
    )
    post, mean = pl.pallas_call(
        functools.partial(main_kernel, sizes),
        out_shape=(
            jax.ShapeDtypeStruct((members, classes, levels), F32),
            jax.ShapeDtypeStruct((classes, levels), F32),
        ),
        in_specs=[SMEM] * 2 + [VMEM] * 5,
        out_specs=(VMEM, VMEM),
        scratch_shapes=[
            pltpu.VMEM((batches, 1, obs), F32),
            pltpu.VMEM((batches, 1, obs), F32),
            pltpu.VMEM((cells, LANES), F32),
            pltpu.VMEM(((batches + 2) * obs, LANES), F32),
            pltpu.VMEM((batches, obs, LANES), F32),
            pltpu.VMEM((obs, 2 * LANES), BF16),
            pltpu.VMEM((2, obs, 2 * LANES), BF16),
            pltpu.VMEM((obs, obs), BF16),
            pltpu.VMEM((obs, obs), BF16),
            pltpu.SemaphoreType.DMA((batches, bands - 1)),
            pltpu.SemaphoreType.DMA((batches, bands - 1)),
        ],
        compiler_params=pltpu.CompilerParams(collective_id=0, has_side_effects=True),
        name="analysis",
    )(
        order, owner, state, rows, obs_cell, root_inv, gain_inv,
    )
    return post.reshape(members, lon_dev, lat_dev, levels), mean.reshape(lon_dev, lat_dev, levels)


def solution(mesh):
    return jax.shard_map(
        local,
        mesh=mesh,
        in_specs=(
            P(None, "gx", "gy", None),
            P("gx", "gy", None),
            P(None, "gy"),
            P(),
            P(),
            P(),
            P(None, "gy", None),
            P(None, "gy", None),
        ),
        out_specs=(P(None, "gx", "gy", None), P("gx", "gy", None)),
        check_vma=False,
    )
```
